256 devices in a mesh: leaf: 8 (over y, core), wide: 32 (over x, z).
Axes of the slice: x: 4, y: 4, z: 8, core: 2. Of those that a mesh axis runs over, the one named last changes fastest.
Arguments:
- rhs: float32 [262144, 256], P(('leaf', 'wide')), may hold values from -6 to 6
- points: float32 [262144, 128], P(('leaf', 'wide')), may hold values from -6 to 6
- order: int32 [262144], P(('leaf', 'wide')), may hold values from 0 to 1023, as said below
- basis: float32 [262144, 256], P(('leaf', 'wide')), may hold values from -0.1875 to 0.1875
- transfer: float32 [256, 256, 256], P(('leaf', 'wide')), may hold values from -0.125 to 0.125
- skeleton: float32 [32, 256, 128], P('wide', 'leaf'), may hold values from -6 to 6
- far_ids: int32 [32, 6], replicated, may hold values from 0 to 31, as said below
- far_count: int32 [32], replicated, may hold values from 1 to 6
- near_ids: int32 [256, 2], P(('leaf', 'wide')), may hold values from 0 to 255, as said below
- near_count: int32 [256], P(('leaf', 'wide')), may hold values from 0 to 2
Outputs:
- product: float32 [262144, 256], P(('leaf', 'wide'))
The draws below stay inside these ranges and needn't reach their ends.
Inputs may be any that keep to these rules, and one draw needn't show every extreme that they name: `order`: within each leaf, the 1024 values are a permutation of 0 to 1023. `far_ids`: the first far_count[p] entries of row p are distinct parents other than p; later entries equal p. `near_ids`: the first near_count[g] entries of row g are distinct and each is g - 1 or g + 1 with the same leaf position, that is, a leaf of the parent beside g's parent; g - 1 comes first; later entries equal g.
All inputs are finite; a program needn't handle non-finite values.
Results may differ from the reference program's by a relative error of at most 0.0003.
Values sent between devices are 32-bit elements; how exact they have to be, the bound alone decides.
A program may use at most 64 MiB of HBM per device.

```python
import jax
import jax.numpy as jnp
from jax import lax

LEAF = 1024
F = 128
RANK = 256
RHS = 256
FAR_MAX = 6
NEAR_MAX = 2
CHILDREN = 8
PARENTS = 32
LEAVES = 256
POINTS = 262144
N_LEAF = 8


def draw_order(key, part):
    keys = jax.random.split(key, LEAVES)
    perms = jax.vmap(lambda single: jax.random.permutation(single, LEAF))(keys)
    return perms.reshape(-1).astype(jnp.int32)


def far_table(key):
    keys = jax.random.split(jax.random.fold_in(key, 11), PARENTS)
    offsets = jax.vmap(lambda single: jax.random.permutation(single, PARENTS - 1)[:FAR_MAX])(keys) + 1
    rows = jnp.arange(PARENTS, dtype=jnp.int32)[:, None]
    ids = (rows + offsets.astype(jnp.int32)) % PARENTS
    counts = jax.random.randint(jax.random.fold_in(key, 12), (PARENTS,), 1, FAR_MAX + 1).astype(jnp.int32)
    counts = counts.at[0].set(FAR_MAX)
    slots = jnp.arange(FAR_MAX, dtype=jnp.int32)[None, :]
    ids = jnp.where(slots < counts[:, None], ids, rows)
    return (ids.astype(jnp.int32), counts)


def draw_far_ids(key, part):
    return far_table(key)[0]


def draw_far_count(key, part):
    return far_table(key)[1]


def near_table(key):
    numbers = jnp.arange(LEAVES, dtype=jnp.int32)
    position = numbers % PARENTS
    bits = jax.random.randint(jax.random.fold_in(key, 21), (LEAVES, 2), 0, 2).astype(jnp.int32)
    take_left = (position > 0) & (bits[:, 0] == 1)
    take_right = (position < PARENTS - 1) & (bits[:, 1] == 1)
    take_left = take_left | (numbers == 1)
    take_right = take_right | (numbers == 1)
    first = jnp.where(take_left, numbers - 1, jnp.where(take_right, numbers + 1, numbers))
    second = jnp.where(take_left & take_right, numbers + 1, numbers)
    counts = take_left.astype(jnp.int32) + take_right.astype(jnp.int32)
    return (jnp.stack([first, second], axis=1).astype(jnp.int32), counts)


def draw_near_ids(key, part):
    return near_table(key)[0]


def draw_near_count(key, part):
    return near_table(key)[1]


def steps_of(own_key, shape, cuts, least, high):
    def one(axis_at, blocks):
        draws = jax.random.uniform(jax.random.fold_in(jax.random.fold_in(own_key, 6), axis_at), (blocks,), jnp.float32, least / len(cuts), high / len(cuts))
        return jnp.repeat(jnp.exp(draws), shape[axis_at] // blocks).reshape((-1,) + (1,) * (len(shape) - axis_at - 1))

    level = one(*cuts[0])
    for cut in cuts[1:]:
        level = level * one(*cut)
    return level


def noise(own_key, dims, spread, reach, cuts=(), held_as=jnp.bfloat16):
    result = jax.random.normal(own_key, dims, jnp.float32) * spread
    if len(cuts) > 0:
        result = steps_of(own_key, dims, cuts, -0.22, 0.18) * result
    return jnp.clip(result, min=-reach, max=reach).astype(held_as)


def setup_inputs(seed: int = 0) -> dict:
    key_of = jax.random.split(jax.random.key(seed), 11)
    return {
        "rhs": noise(key_of[0], (POINTS, RHS), 1.0, 6.0, ((0, 256),), jnp.float32),
        "points": noise(key_of[1], (POINTS, F), 1.0, 6.0, ((0, 256),), jnp.float32),
        "order": draw_order(jax.random.fold_in(key_of[10], 71), 0),
        "basis": noise(key_of[3], (POINTS, RANK), LEAF ** -0.5, 0.1875, ((0, 256),), jnp.float32),
        "transfer": noise(key_of[4], (LEAVES, RANK, RANK), (RANK * CHILDREN) ** -0.5, 0.125, ((0, 256),), jnp.float32),
        "skeleton": noise(key_of[5], (PARENTS, RANK, F), 1.0, 6.0, ((0, 32), (1, 8)), jnp.float32),
        "far_ids": draw_far_ids(jax.random.fold_in(key_of[10], 71), 0),
        "far_count": draw_far_count(jax.random.fold_in(key_of[10], 71), 0),
        "near_ids": draw_near_ids(jax.random.fold_in(key_of[10], 71), 0),
        "near_count": draw_near_count(jax.random.fold_in(key_of[10], 71), 0),
    }


HIGH = lax.Precision.HIGHEST


def multiply(left, right):
    return lax.dot_general(left, right, (((1,), (0,)), ((), ())), precision=HIGH, preferred_element_type=jnp.float32)


def kernel_tile(left, right):
    cross = lax.dot_general(left, right, (((1,), (1,)), ((), ())), precision=HIGH, preferred_element_type=jnp.float32)
    sq_left = jnp.sum(left * left, axis=1)
    sq_right = jnp.sum(right * right, axis=1)
    return jnp.exp((-2.0 / left.shape[1]) * (sq_left[:, None] + sq_right[None, :] - 2.0 * cross))


def reference(rhs, points, order, basis, transfer, skeleton, far_ids, far_count, near_ids, near_count):
    index = (jnp.arange(LEAVES, dtype=jnp.int32)[:, None] * LEAF + order.reshape(LEAVES, LEAF)).reshape(-1)
    tree_rhs = rhs[index]
    rhs_blocks = tree_rhs.reshape(LEAVES, LEAF, RHS)
    point_blocks = points.reshape(LEAVES, LEAF, F)
    basis_blocks = basis.reshape(LEAVES, LEAF, RANK)
    leaf_coef = jnp.einsum("lpr,lpc->lrc", basis_blocks, rhs_blocks, precision=HIGH)
    lifted = jnp.einsum("lrs,lrc->lsc", transfer, leaf_coef, precision=HIGH)
    parent_coef = jnp.sum(lifted.reshape(N_LEAF, PARENTS, RANK, RHS), axis=0)

    def far_one(parent):
        total = jnp.zeros((RANK, RHS), jnp.float32)
        for slot in range(FAR_MAX):
            other = far_ids[parent, slot]
            term = multiply(kernel_tile(skeleton[parent], skeleton[other]), parent_coef[other])
            total = total + jnp.where(slot < far_count[parent], term, jnp.float32(0.0))
        return total

    parent_field = lax.map(far_one, jnp.arange(PARENTS, dtype=jnp.int32))
    owners = jnp.arange(LEAVES, dtype=jnp.int32) % PARENTS
    leaf_field = jnp.einsum("lrs,lsc->lrc", transfer, parent_field[owners], precision=HIGH)

    def near_one(leaf_number):
        own_points = point_blocks[leaf_number]
        total = multiply(kernel_tile(own_points, own_points), rhs_blocks[leaf_number])
        for slot in range(NEAR_MAX):
            source = near_ids[leaf_number, slot]
            total = total + lax.cond(
                slot < near_count[leaf_number],
                lambda: multiply(kernel_tile(own_points, point_blocks[source]), rhs_blocks[source]),
                lambda: jnp.zeros((LEAF, RHS), jnp.float32))
        return total + multiply(basis_blocks[leaf_number], leaf_field[leaf_number])

    tree_out = lax.map(near_one, jnp.arange(LEAVES, dtype=jnp.int32)).reshape(POINTS, RHS)
    return jnp.zeros_like(rhs).at[index].set(tree_out)
```

```python
import jax
import jax.numpy as jnp
from jax import lax
from jax.experimental import pallas as pl
from jax.experimental.pallas import tpu as pltpu
from jax.sharding import PartitionSpec as P

MESH = pl.DeviceIdType.MESH
F32, BF16 = jnp.float32, jnp.bfloat16
LEAVES, WIDE, NX, NZ = 8, 32, 4, 8
ROWS, FEAT, RANK, COLS = 1024, 128, 256, 256
FAR, PART = 6, 32
BLOCK = 256
STEPS = ROWS // BLOCK
RHS_CHUNK = 128
COPIES = 96
SCALE = -(2.0 / FEAT) * 1.4426950408889634

LAST = (((1,), (1,)), ((), ()))
FIRST = (((0,), (0,)), ((), ()))
PLAIN = (((1,), (0,)), ((), ()))


def dot(a, b, dims=PLAIN):
    return lax.dot_general(a, b, dims, preferred_element_type=F32)


def split(x):
    high = x.astype(BF16)
    return high, (x - high.astype(F32)).astype(BF16)


def dot3(a, b, dims=PLAIN):
    return dot(a[0], b[0], dims) + (dot(a[0], b[1], dims) + dot(a[1], b[0], dims))


def kernel(
    order, far_ids, far_count, near_ids, near_count, rhs, points, basis, transfer, skeleton, out,
    moved, q, own_hl, own_lh, own_col, own_row, q_in, in_hl, in_lh, in_col, in_row,
    basis_h, basis_l, rhs_h, rhs_l, rhs_in, in_h, in_l, share_out, share_in,
    lifted, pieces, coefs, skel_parent, skels, chosen_out, chosen, tile_h, tile_l, field,
    send_sems, recv_sems,
):
    leaf, wide = lax.axis_index("leaf"), lax.axis_index("wide")
    x, z = lax.div(wide, NZ), lax.rem(wide, NZ)
    step = 2 * lax.rem(leaf, 2) - 1
    ahead, behind = lax.rem(wide + step + WIDE, WIDE), lax.rem(wide - step + WIDE, WIDE)

    def leaf_peer(d):
        return lax.rem(leaf + d, LEAVES), wide

    def z_peer(d):
        return leaf, x * NZ + lax.rem(z + d, NZ)

    def x_peer(d):
        return leaf, lax.rem(x + d, NX) * NZ + z

    barrier = pltpu.get_barrier_semaphore()
    partners = [leaf_peer(d) for d in range(1, LEAVES)] + [z_peer(d) for d in range(1, NZ)]
    partners += [x_peer(d) for d in range(1, NX)] + [(leaf, ahead), (leaf, behind)]
    for partner in partners:
        pl.semaphore_signal(barrier, inc=1, device_id=partner, device_id_type=MESH)
    pl.semaphore_wait(barrier, len(partners))

    copies = []

    def send(src, dst, partner):
        k = len(copies)
        copy = pltpu.make_async_remote_copy(
            src_ref=src, dst_ref=dst, send_sem=send_sems.at[k], recv_sem=recv_sems.at[k],
            device_id=partner, device_id_type=MESH)
        copy.start()
        copies.append(copy)
        return copy

    skel_leaf = [send(skeleton.at[0], skel_parent.at[leaf], leaf_peer(d)) for d in range(1, LEAVES)]
    skel_z = [send(skeleton.at[0], skels.at[wide], z_peer(d)) for d in range(1, NZ)]
    skel_parent[leaf] = skeleton[0]
    skels[wide] = skeleton[0]

    def send_rhs(first, last):
        return [
            send(rhs.at[pl.ds(i * RHS_CHUNK, RHS_CHUNK)], rhs_in.at[pl.ds(i * RHS_CHUNK, RHS_CHUNK)], (leaf, ahead))
            for i in range(first, last)]

    near_rhs = send_rhs(0, 2)

    moved[:, 0:128], moved[:, 128:256] = split(points[...])
    moved[:, 256:512], moved[:, 512:768] = split(basis[...])
    rhs_h[...], rhs_l[...] = split(rhs[...])

    def reorder(i, carry):
        rows = pl.ds(pl.multiple_of(i * BLOCK, BLOCK), BLOCK)
        place = lax.broadcasted_iota(jnp.int32, (BLOCK, ROWS), 0) + i * BLOCK
        chosen_rows = jnp.where(order[...] == place, 1.0, 0.0).astype(BF16)
        got = dot(chosen_rows, moved[...])
        high, low = got[:, 0:128], got[:, 128:256]
        q[rows, :] = high + low
        own_hl[rows, 0:128] = high.astype(BF16)
        own_hl[rows, 128:256] = low.astype(BF16)
        own_lh[rows, 0:128] = low.astype(BF16)
        own_lh[rows, 128:256] = high.astype(BF16)
        basis_h[rows, :] = got[:, 256:512].astype(BF16)
        basis_l[rows, :] = got[:, 512:768].astype(BF16)
        return carry

    lax.fori_loop(0, STEPS, reorder, 0)
    near_q = [
        send(q.at[pl.ds(i * BLOCK, BLOCK)], q_in.at[pl.ds(i * BLOCK, BLOCK)], (leaf, ahead)) for i in range(STEPS)]
    near_rhs += send_rhs(2, 4)

    basis_hl = (basis_h[...], basis_l[...])
    leaf_coef = dot3((rhs_h[...], rhs_l[...]), basis_hl, FIRST)
    transfer_hl = split(transfer[0])
    lifted[...] = dot3(split(leaf_coef), transfer_hl)
    piece = [
        send(lifted.at[pl.ds(pl.multiple_of(leaf_peer(d)[0] * PART, PART), PART)], pieces.at[leaf], leaf_peer(d))
        for d in range(1, LEAVES)]
    pieces[leaf] = lifted[pl.ds(pl.multiple_of(leaf * PART, PART), PART), :]

    for copy in skel_z:
        copy.wait_recv()
    rows_of_x = pl.ds(x * NZ, NZ)
    skel_x = [send(skels.at[rows_of_x], skels.at[rows_of_x], x_peer(d)) for d in range(1, NX)]

    def norms(points_ref, column, row):
        sq = SCALE * jnp.sum(points_ref[...] * points_ref[...], axis=1, keepdims=True)
        column[...] = sq
        row[...] = jnp.transpose(jnp.broadcast_to(sq, (sq.shape[0], 128)))[0:1, :]

    def tile(left, left_col, right_hl, right_lh, right_row):
        cross = dot(left, right_hl, LAST) + dot(left, right_lh, LAST)
        return split(jnp.exp2((left_col + right_row) - (2.0 * SCALE) * cross))

    norms(q, own_col, own_row)

    def own_term(i, carry):
        rows = pl.ds(pl.multiple_of(i * BLOCK, BLOCK), BLOCK)
        t = tile(own_hl[rows, :], own_col[rows, :], own_hl[...], own_lh[...], own_row[...])
        out[rows, :] = dot3(t, (rhs_h[...], rhs_l[...]))
        return carry

    lax.fori_loop(0, STEPS, own_term, 0)

    for copy in piece:
        copy.wait_recv()
    coefs[wide] = jnp.sum(pieces[...], axis=0)
    coef_z = [send(coefs.at[wide], coefs.at[wide], z_peer(d)) for d in range(1, NZ)]
    coef_x = [send(coefs.at[wide], coefs.at[wide], x_peer(d)) for d in range(1, NX)]
    near_rhs += send_rhs(4, 8)

    for copy in skel_x:
        copy.wait_recv()
    for j in range(FAR):
        chosen_out[j] = skels[far_ids[wide, j]]
    chosen[:, leaf] = chosen_out[...]
    picked = [send(chosen_out, chosen.at[:, leaf], leaf_peer(d)) for d in range(1, LEAVES)]

    for copy in near_q:
        copy.wait_recv()
    high, low = split(q_in[...])
    in_hl[:, 0:128], in_hl[:, 128:256] = high, low
    in_lh[:, 0:128], in_lh[:, 128:256] = low, high
    norms(q_in, in_col, in_row)
    shares = []
    for i in range(STEPS):
        rows = pl.ds(i * BLOCK, BLOCK)
        t = tile(in_hl[rows, :], in_col[rows, :], own_hl[...], own_lh[...], own_row[...])
        share_out[rows, :] = dot3(t, (rhs_h[...], rhs_l[...]))
        shares.append(send(share_out.at[rows], share_in.at[rows], (leaf, behind)))
        for d in ((1, 7), (2, 6), (3, 5), (4,))[i]:
            coef_z[d - 1].wait_recv()
            block = coefs.at[x * NZ + lax.rem(z - d + NZ, NZ)]
            coef_x += [send(block, block, x_peer(e)) for e in range(1, NX)]

    first_id, second_id, used = near_ids[0, 0], near_ids[0, 1], near_count[0]
    number = leaf * WIDE + wide

    def listed(other):
        return jnp.where(((first_id == other) & (used > 0)) | ((second_id == other) & (used > 1)), 1.0, 0.0).astype(F32)

    behind_used, ahead_used = listed(number - step), listed(number + step)

    for copy in near_rhs:
        copy.wait_recv()
    in_h[...], in_l[...] = split(rhs_in[...])

    def near_term(i, carry):
        rows = pl.ds(pl.multiple_of(i * BLOCK, BLOCK), BLOCK)
        t = tile(own_hl[rows, :], own_col[rows, :], in_hl[...], in_lh[...], in_row[...])
        out[rows, :] += behind_used * dot3(t, (in_h[...], in_l[...]))
        return carry

    lax.fori_loop(0, STEPS, near_term, 0)

    for copy in picked + skel_leaf:
        copy.wait_recv()
    targets = skel_parent[...].reshape(RANK, FEAT)
    target_high, target_low = split(targets)
    target_hl = jnp.concatenate([target_high, target_low], axis=1)
    target_lh = jnp.concatenate([target_low, target_high], axis=1)
    target_sq = SCALE * jnp.sum(targets * targets, axis=1, keepdims=True)
    target_row = jnp.transpose(jnp.broadcast_to(target_sq, (RANK, 128)))[0:1, :]
    for j in range(FAR):
        sources = chosen[j].reshape(RANK, FEAT)
        source_sq = SCALE * jnp.sum(sources * sources, axis=1, keepdims=True)
        tile_h[j], tile_l[j] = tile(
            jnp.concatenate(split(sources), axis=1), source_sq, target_hl, target_lh, target_row)

    for copy in coef_x:
        copy.wait_recv()
    total = jnp.zeros((PART, RANK), F32)
    for j in range(FAR):
        mask = jnp.where(far_count[wide] > j, 1.0, 0.0).astype(F32)
        total += mask * dot3(split(coefs[far_ids[wide, j]]), (tile_h[j], tile_l[j]))
    field[leaf] = total
    fields = [send(field.at[leaf], field.at[leaf], leaf_peer(d)) for d in range(1, LEAVES)]
    for copy in fields:
        copy.wait_recv()
    leaf_field = dot3(split(field[...].reshape(COLS, RANK)), transfer_hl, LAST)
    far_out = dot3((basis_h[...], basis_l[...]), split(leaf_field), LAST)

    for copy in shares:
        copy.wait_recv()
    out[...] += far_out + ahead_used * share_in[...]
    for copy in copies:
        copy.wait_send()


def shards(rhs, points, order, basis, transfer, skeleton, far_ids, far_count, near_ids, near_count):
    vmem, smem = pl.BlockSpec(memory_space=pltpu.VMEM), pl.BlockSpec(memory_space=pltpu.SMEM)

    def held(*shape, dtype=F32):
        return pltpu.VMEM(shape, dtype)

    wide_bf16 = held(ROWS, 256, dtype=BF16)
    return pl.pallas_call(
        kernel,
        out_shape=jax.ShapeDtypeStruct((ROWS, COLS), F32),
        in_specs=[vmem, smem, smem, smem, smem] + [vmem] * 5,
        out_specs=vmem,
        scratch_shapes=[
            held(ROWS, 768, dtype=BF16),
            held(ROWS, FEAT), wide_bf16, wide_bf16, held(ROWS, 1), held(1, ROWS),
            held(ROWS, FEAT), wide_bf16, wide_bf16, held(ROWS, 1), held(1, ROWS),
            wide_bf16, wide_bf16, wide_bf16, wide_bf16,
            held(ROWS, COLS), wide_bf16, wide_bf16,
            held(ROWS, COLS), held(ROWS, COLS),
            held(COLS, RANK), held(LEAVES, PART, RANK), held(WIDE, PART, RANK),
            held(LEAVES, PART, FEAT), held(WIDE, PART, FEAT),
            held(FAR, PART, FEAT), held(FAR, LEAVES, PART, FEAT),
            held(FAR, RANK, RANK, dtype=BF16), held(FAR, RANK, RANK, dtype=BF16),
            held(LEAVES, PART, RANK),
            pltpu.SemaphoreType.DMA((COPIES,)),
            pltpu.SemaphoreType.DMA((COPIES,)),
        ],
        compiler_params=pltpu.CompilerParams(
            collective_id=0, has_side_effects=True, vmem_limit_bytes=56 * 1024 * 1024),
    )(order.reshape(1, ROWS), far_ids, far_count, near_ids, near_count, rhs, points, basis, transfer, skeleton)


def solution(mesh):
    placed = (
        P(("leaf", "wide"), None),
        P(("leaf", "wide"), None),
        P(("leaf", "wide")),
        P(("leaf", "wide"), None),
        P(("leaf", "wide"), None, None),
        P("wide", "leaf", None),
        P(),
        P(),
        P(("leaf", "wide"), None),
        P(("leaf", "wide")),
    )
    return jax.shard_map(
        shards, mesh=mesh, in_specs=placed, out_specs=P(("leaf", "wide"), None), check_vma=False
    )
```

```python
import jax
import jax.numpy as jnp
from jax import lax
from jax.experimental import pallas as pl
from jax.experimental.pallas import tpu as pltpu
from jax.sharding import PartitionSpec as P

MESH = pl.DeviceIdType.MESH
F32, BF16 = jnp.float32, jnp.bfloat16
LEAVES, WIDE, NX, NZ = 8, 32, 4, 8
ROWS, FEAT, RANK, COLS = 1024, 128, 256, 256
FAR, PART = 6, 32
BLOCK = 256
STEPS = ROWS // BLOCK
RHS_CHUNK = 128
COPIES = 128
SCALE = -(2.0 / FEAT) * 1.4426950408889634

LAST = (((1,), (1,)), ((), ()))
FIRST = (((0,), (0,)), ((), ()))
PLAIN = (((1,), (0,)), ((), ()))


def dot(a, b, dims=PLAIN):
    return lax.dot_general(a, b, dims, preferred_element_type=F32)


def split(x):
    high = x.astype(BF16)
    return high, (x - high.astype(F32)).astype(BF16)


def dot3(a, b, dims=PLAIN):
    return dot(a[0], b[0], dims) + (dot(a[0], b[1], dims) + dot(a[1], b[0], dims))


def kernel(
    order, far_ids, far_count, near_ids, near_count, rhs_hbm, points_hbm, basis_hbm, transfer_hbm, skeleton,
    out, share,
    rhs, points, basis, transfer,
    moved, q, own_hl, own_lh, own_col, own_row, q_in, in_hl, in_lh, in_col, in_row,
    basis_h, basis_l, rhs_h, rhs_l, rhs_in, in_h, in_l, share_out, share_in,
    lifted, half, pieces, coefs, skel_parent, skels, chosen, tile_h, tile_l, field,
    load_sems, send_sems, recv_sems,
):
    leaf, wide = lax.axis_index("leaf"), lax.axis_index("wide")
    core, chip = lax.rem(leaf, 2), lax.div(leaf, 2)
    x, z = lax.div(wide, NZ), lax.rem(wide, NZ)
    step = 2 * core - 1
    ahead, behind = lax.rem(wide + step + WIDE, WIDE), lax.rem(wide - step + WIDE, WIDE)
    way = 2 * lax.div(z, NZ - 1) - 1

    def leaf_peer(d):
        return lax.rem(leaf + d, LEAVES), wide

    def z_index(d):
        return x * NZ + lax.rem(z + d + NZ, NZ)

    def x_index(d):
        return lax.rem(x + d + 3 * NX, NX) * NZ

    loads = []
    for source, target in ((rhs_hbm, rhs), (points_hbm, points), (basis_hbm, basis), (transfer_hbm, transfer)):
        load = pltpu.make_async_copy(source, target, load_sems.at[len(loads)])
        load.start()
        loads.append(load)

    barrier = pltpu.get_barrier_semaphore()
    partners = [leaf_peer(d) for d in range(1, LEAVES)] + [(leaf, z_index(d)) for d in range(1, NZ)]
    partners += [(leaf, x_index(1) + z), (leaf, x_index(-1) + z), (leaf, ahead), (leaf, behind)]
    for partner in partners:
        pl.semaphore_signal(barrier, inc=1, device_id=partner, device_id_type=MESH)
    pl.semaphore_wait(barrier, len(partners))

    copies = []

    def send(src, dst, partner):
        k = len(copies)
        copy = pltpu.make_async_remote_copy(
            src_ref=src, dst_ref=dst, send_sem=send_sems.at[k], recv_sem=recv_sems.at[k],
            device_id=partner, device_id_type=MESH)
        copy.start()
        copies.append(copy)
        return copy

    def arrived(group):
        for copy in group:
            copy.wait_recv()

    FARTHEST_FIRST = (4, 3, -3, 2, -2, 1, -1)

    def along_z(buffer):
        block = buffer.at[wide]
        return {d: send(block, block, (leaf, z_index(d))) for d in FARTHEST_FIRST}

    def to_x_neighbours(blocks):
        return [send(blocks, blocks, (leaf, x_index(d) + z)) for d in (way, -way)]

    def passed_on(sent, blocks):
        sent[0].wait_recv()
        return [sent[1], send(blocks, blocks, (leaf, x_index(way) + z))]

    skels[wide] = skeleton[0]
    skel_z = list(along_z(skels).values())
    skel_leaf = [send(skeleton.at[0], skel_parent.at[leaf], leaf_peer(d)) for d in range(1, LEAVES)]
    skel_parent[leaf] = skeleton[0]

    near_rhs, near_q, shares = [], [], []

    def send_rhs(count):
        for _ in range(count):
            rows = pl.ds(len(near_rhs) * RHS_CHUNK, RHS_CHUNK)
            near_rhs.append(send(rhs.at[rows], rhs_in.at[rows], (leaf, ahead)))

    loads[0].wait()
    send_rhs(3)
    rhs_h[...], rhs_l[...] = split(rhs[...])
    loads[1].wait()
    loads[2].wait()

    moved[:, 0:128], moved[:, 128:256] = split(points[...])
    moved[:, 256:512], moved[:, 512:768] = split(basis[...])

    def reorder(i, carry):
        rows = pl.ds(pl.multiple_of(i * BLOCK, BLOCK), BLOCK)
        place = lax.broadcasted_iota(jnp.int32, (BLOCK, ROWS), 0) + i * BLOCK
        chosen_rows = jnp.where(order[...] == place, 1.0, 0.0).astype(BF16)
        got = dot(chosen_rows, moved[...])
        high, low = got[:, 0:128], got[:, 128:256]
        q[rows, :] = high + low
        own_hl[rows, 0:128] = high.astype(BF16)
        own_hl[rows, 128:256] = low.astype(BF16)
        own_lh[rows, 0:128] = low.astype(BF16)
        own_lh[rows, 128:256] = high.astype(BF16)
        basis_h[rows, :] = got[:, 256:512].astype(BF16)
        basis_l[rows, :] = got[:, 512:768].astype(BF16)
        return carry

    lax.fori_loop(0, STEPS, reorder, 0)
    for i in range(STEPS):
        rows = pl.ds(i * BLOCK, BLOCK)
        near_q.append(send(q.at[rows], q_in.at[rows], (leaf, ahead)))

    leaf_coef = dot3((rhs_h[...], rhs_l[...]), (basis_h[...], basis_l[...]), FIRST)
    loads[3].wait()
    transfer_hl = split(transfer[0])
    lifted[...] = dot3(split(leaf_coef), transfer_hl).reshape(LEAVES // 2, 2, PART, RANK)
    halved = [send(lifted.at[:, 1 - core], half.at[:, 0], (leaf - step, wide))]

    def norms(points_ref, column, row):
        sq = SCALE * jnp.sum(points_ref[...] * points_ref[...], axis=1, keepdims=True)
        column[...] = sq
        row[...] = jnp.transpose(jnp.broadcast_to(sq, (sq.shape[0], 128)))[0:1, :]

    def tile(left, left_col, right_hl, right_lh, right_row):
        cross = dot(left, right_hl, LAST) + dot(left, right_lh, LAST)
        return split(jnp.exp2((left_col + right_row) - (2.0 * SCALE) * cross))

    def own_term(i, carry):
        rows = pl.ds(pl.multiple_of(i * BLOCK, BLOCK), BLOCK)
        t = tile(own_hl[rows, :], own_col[rows, :], own_hl[...], own_lh[...], own_row[...])
        out[rows, :] = dot3(t, (rhs_h[...], rhs_l[...]))
        return carry

    norms(q, own_col, own_row)
    arrived(halved)
    half[:, 1] = half[:, 0] + lifted[:, core]
    pieces[chip] = half[chip, 1]
    piece = []
    for d in (2, 1, 3):
        other = lax.rem(chip + d, LEAVES // 2)
        piece.append(send(half.at[other, 1], pieces.at[chip], (2 * other + core, wide)))
    own_rows = pl.ds(x * NZ, NZ)
    arrived(skel_z)
    skel_x = to_x_neighbours(skels.at[own_rows])
    lax.fori_loop(0, STEPS, own_term, 0)

    arrived(piece)
    coefs[wide] = jnp.sum(pieces[...], axis=0)
    coef_z = along_z(coefs)
    coef_x = {0: to_x_neighbours(coefs.at[wide])}
    send_rhs(2)
    skel_x = passed_on(skel_x, skels.at[pl.ds(x_index(-way), NZ)])

    def along_x(*offsets):
        for d in offsets:
            coef_z[d].wait_recv()
            coef_x[d] = to_x_neighbours(coefs.at[z_index(-d)])

    def onward(*offsets):
        for d in offsets:
            coef_x[d] = passed_on(coef_x[d], coefs.at[x_index(-way) + lax.rem(z - d + NZ, NZ)])

    arrived(near_q)
    high, low = split(q_in[...])
    in_hl[:, 0:128], in_hl[:, 128:256] = high, low
    in_lh[:, 0:128], in_lh[:, 128:256] = low, high
    norms(q_in, in_col, in_row)

    def share_term(i):
        rows = pl.ds(i * BLOCK, BLOCK)
        t = tile(in_hl[rows, :], in_col[rows, :], own_hl[...], own_lh[...], own_row[...])
        share_out[rows, :] = dot3(t, (rhs_h[...], rhs_l[...]))
        shares.append(send(share_out.at[rows], share_in.at[rows], (leaf, behind)))

    share_term(0)
    along_x(1, -1, 2, -2)
    send_rhs(1)
    share_term(1)
    along_x(3, -3, 4)
    send_rhs(2)
    onward(0)
    share_term(2)
    onward(1, -1, 2, -2)

    arrived(skel_x)
    for j in range(FAR):
        chosen[chip, core, j] = skels[far_ids[j, wide]]
    picked = [send(chosen.at[chip, core], chosen.at[chip, core], leaf_peer(d)) for d in (2, 4, 6)]
    share_term(3)
    onward(3, -3, 4)

    first_id, second_id, used = near_ids[0, 0], near_ids[0, 1], near_count[0]
    number = leaf * WIDE + wide

    def listed(other):
        return jnp.where(((first_id == other) & (used > 0)) | ((second_id == other) & (used > 1)), 1.0, 0.0).astype(F32)

    behind_used, ahead_used = listed(number - step), listed(number + step)

    arrived(near_rhs)
    in_h[...], in_l[...] = split(rhs_in[...])

    def near_term(i, carry):
        rows = pl.ds(pl.multiple_of(i * BLOCK, BLOCK), BLOCK)
        t = tile(own_hl[rows, :], own_col[rows, :], in_hl[...], in_lh[...], in_row[...])
        out[rows, :] += behind_used * dot3(t, (in_h[...], in_l[...]))
        return carry

    lax.fori_loop(0, 2, near_term, 0)
    arrived(picked)
    picked = [send(chosen.at[:, core], chosen.at[:, core], (leaf - step, wide))]
    lax.fori_loop(2, STEPS, near_term, 0)

    arrived(picked + skel_leaf)
    targets = skel_parent[...].reshape(RANK, FEAT)
    target_high, target_low = split(targets)
    target_hl = jnp.concatenate([target_high, target_low], axis=1)
    target_lh = jnp.concatenate([target_low, target_high], axis=1)
    target_sq = SCALE * jnp.sum(targets * targets, axis=1, keepdims=True)
    target_row = jnp.transpose(jnp.broadcast_to(target_sq, (RANK, 128)))[0:1, :]
    for j in range(FAR):
        sources = chosen[:, :, j].reshape(RANK, FEAT)
        source_sq = SCALE * jnp.sum(sources * sources, axis=1, keepdims=True)
        tile_h[j], tile_l[j] = tile(
            jnp.concatenate(split(sources), axis=1), source_sq, target_hl, target_lh, target_row)

    for group in coef_x.values():
        arrived(group)
    total = jnp.zeros((PART, RANK), F32)
    for j in range(FAR):
        mask = jnp.where(far_count[wide] > j, 1.0, 0.0).astype(F32)
        total += mask * dot3(split(coefs[far_ids[j, wide]]), (tile_h[j], tile_l[j]))
    field[chip, core] = total
    partner = (leaf - step, wide)
    fields = [send(field.at[chip, core], field.at[chip, core], leaf_peer(d)) for d in (4, 2, 6)]
    inside = [send(field.at[chip, core], field.at[chip, core], partner)]
    arrived(shares)
    share[...] = ahead_used * share_in[...]
    for copy, d in ((fields[1], 2), (fields[2], 6), (fields[0], 4)):
        copy.wait_recv()
        block = field.at[lax.rem(chip + LEAVES // 2 - d // 2, LEAVES // 2), core]
        inside.append(send(block, block, partner))
    arrived(inside)
    leaf_field = dot3(split(field[...].reshape(COLS, RANK)), transfer_hl, LAST)
    out[...] += dot3((basis_h[...], basis_l[...]), split(leaf_field), LAST)
    for copy in copies:
        copy.wait_send()


def shards(rhs, points, order, basis, transfer, skeleton, far_ids, far_count, near_ids, near_count):
    vmem, smem, anywhere = (pl.BlockSpec(memory_space=m) for m in (pltpu.VMEM, pltpu.SMEM, pl.ANY))

    def held(*shape, dtype=F32):
        return pltpu.VMEM(shape, dtype)

    wide_bf16 = held(ROWS, 256, dtype=BF16)
    total, share = pl.pallas_call(
        kernel,
        out_shape=(jax.ShapeDtypeStruct((ROWS, COLS), F32), jax.ShapeDtypeStruct((ROWS, COLS), F32)),
        in_specs=[vmem, smem, smem, smem, smem] + [anywhere] * 4 + [vmem],
        out_specs=(vmem, vmem),
        scratch_shapes=[
            held(ROWS, COLS), held(ROWS, FEAT), held(ROWS, RANK), held(1, RANK, RANK),
            held(ROWS, 768, dtype=BF16),
            held(ROWS, FEAT), wide_bf16, wide_bf16, held(ROWS, 1), held(1, ROWS),
            held(ROWS, FEAT), wide_bf16, wide_bf16, held(ROWS, 1), held(1, ROWS),
            wide_bf16, wide_bf16, wide_bf16, wide_bf16,
            held(ROWS, COLS), wide_bf16, wide_bf16,
            held(ROWS, COLS), held(ROWS, COLS),
            held(LEAVES // 2, 2, PART, RANK), held(LEAVES // 2, 2, PART, RANK),
            held(LEAVES // 2, PART, RANK), held(WIDE, PART, RANK),
            held(LEAVES, PART, FEAT), held(WIDE, PART, FEAT),
            held(LEAVES // 2, 2, FAR, PART, FEAT),
            held(FAR, RANK, RANK, dtype=BF16), held(FAR, RANK, RANK, dtype=BF16),
            held(LEAVES // 2, 2, PART, RANK),
            pltpu.SemaphoreType.DMA((4,)),
            pltpu.SemaphoreType.DMA((COPIES,)),
            pltpu.SemaphoreType.DMA((COPIES,)),
        ],
        compiler_params=pltpu.CompilerParams(
            collective_id=0, has_side_effects=True, vmem_limit_bytes=56 * 1024 * 1024),
    )(order.reshape(1, ROWS), far_ids.T, far_count, near_ids, near_count, rhs, points, basis, transfer, skeleton)
    return total + share


def solution(mesh):
    placed = (
        P(("leaf", "wide"), None),
        P(("leaf", "wide"), None),
        P(("leaf", "wide")),
        P(("leaf", "wide"), None),
        P(("leaf", "wide"), None, None),
        P("wide", "leaf", None),
        P(),
        P(),
        P(("leaf", "wide"), None),
        P(("leaf", "wide")),
    )
    return jax.shard_map(
        shards, mesh=mesh, in_specs=placed, out_specs=P(("leaf", "wide"), None), check_vma=False
    )
```

```python
import jax
import jax.numpy as jnp
from jax import lax
from jax.experimental import pallas as pl
from jax.experimental.pallas import tpu as pltpu
from jax.sharding import PartitionSpec as P

MESH = pl.DeviceIdType.MESH
F32, BF16 = jnp.float32, jnp.bfloat16
LEAVES, WIDE, NX, NZ = 8, 32, 4, 8
ROWS, FEAT, RANK, COLS = 1024, 128, 256, 256
FAR, PART = 6, 32
BLOCK = 256
STEPS = ROWS // BLOCK
RHS_CHUNK = 128
COPIES = 128
SCALE = -(2.0 / FEAT) * 1.4426950408889634

LAST = (((1,), (1,)), ((), ()))
FIRST = (((0,), (0,)), ((), ()))
PLAIN = (((1,), (0,)), ((), ()))
FARTHEST_FIRST = (4, 3, -3, 2, -2, 1, -1)


def dot(a, b, dims=PLAIN):
    return lax.dot_general(a, b, dims, preferred_element_type=F32)


def split(x):
    high = x.astype(BF16)
    return high, (x - high.astype(F32)).astype(BF16)


def dot3(a, b, dims=PLAIN):
    return dot(a[0], b[0], dims) + (dot(a[0], b[1], dims) + dot(a[1], b[0], dims))


def kernel(
    order, far_ids, far_count, near_ids, near_count, rhs_hbm, points_hbm, basis_hbm, transfer_hbm, skeleton,
    out, share,
    rhs, points, basis, transfer,
    moved, q, own_hl, own_lh, own_col, own_row, q_in, in_hl, in_lh, in_col, in_row,
    basis_h, basis_l, rhs_h, rhs_l, rhs_in, in_h, in_l, share_out, share_in,
    lifted, half, pieces, coefs, skels, far_points, far_hl, far_lh, far_col, far_row, tile_h, tile_l,
    parts_out, parts_in, field,
    load_sems, send_sems, recv_sems,
):
    leaf, wide = lax.axis_index("leaf"), lax.axis_index("wide")
    core, chip = lax.rem(leaf, 2), lax.div(leaf, 2)
    x, z = lax.div(wide, NZ), lax.rem(wide, NZ)
    step = 2 * core - 1
    ahead, behind = lax.rem(wide + step + WIDE, WIDE), lax.rem(wide - step + WIDE, WIDE)

    def leaf_peer(d):
        return lax.rem(leaf + d, LEAVES), wide

    def z_index(d):
        return x * NZ + lax.rem(z + d + NZ, NZ)

    def x_index(d):
        return lax.rem(x + d + 3 * NX, NX) * NZ

    loads = []
    for source, target in ((rhs_hbm, rhs), (points_hbm, points), (basis_hbm, basis), (transfer_hbm, transfer)):
        load = pltpu.make_async_copy(source, target, load_sems.at[len(loads)])
        load.start()
        loads.append(load)

    barrier = pltpu.get_barrier_semaphore()
    partners = [leaf_peer(d) for d in range(1, LEAVES)] + [(leaf, z_index(d)) for d in range(1, NZ)]
    partners += [(leaf, x_index(d) + z) for d in range(1, NX)] + [(leaf, ahead), (leaf, behind)]
    for partner in partners:
        pl.semaphore_signal(barrier, inc=1, device_id=partner, device_id_type=MESH)
    pl.semaphore_wait(barrier, len(partners))

    copies = []

    def send(src, dst, partner):
        k = len(copies)
        copy = pltpu.make_async_remote_copy(
            src_ref=src, dst_ref=dst, send_sem=send_sems.at[k], recv_sem=recv_sems.at[k],
            device_id=partner, device_id_type=MESH)
        copy.start()
        copies.append(copy)
        return copy

    def arrived(group):
        for copy in group:
            copy.wait_recv()

    FARTHEST_FIRST = (4, 3, -3, 2, -2, 1, -1)

    own_set = skels.at[chip, core]
    partner = (leaf - step, wide)
    skel_row = [send(skeleton.at[0], own_set.at[z], (leaf, z_index(d))) for d in FARTHEST_FIRST]
    skel_row += [send(skeleton.at[0], own_set.at[NZ + x], (leaf, x_index(d) + z)) for d in (2, 1, 3)]
    skels[chip, core, z] = skeleton[0]
    skels[chip, core, NZ + x] = skeleton[0]

    near_rhs, near_q, shares = [], [], []

    def send_rhs(count):
        for _ in range(count):
            rows = pl.ds(len(near_rhs) * RHS_CHUNK, RHS_CHUNK)
            near_rhs.append(send(rhs.at[rows], rhs_in.at[rows], (leaf, ahead)))

    loads[0].wait()
    send_rhs(3)
    rhs_h[...], rhs_l[...] = split(rhs[...])
    loads[1].wait()
    loads[2].wait()

    moved[:, 0:128], moved[:, 128:256] = split(points[...])
    moved[:, 256:512], moved[:, 512:768] = split(basis[...])

    def reorder(i, carry):
        rows = pl.ds(pl.multiple_of(i * BLOCK, BLOCK), BLOCK)
        place = lax.broadcasted_iota(jnp.int32, (BLOCK, ROWS), 0) + i * BLOCK
        chosen_rows = jnp.where(order[...] == place, 1.0, 0.0).astype(BF16)
        got = dot(chosen_rows, moved[...])
        high, low = got[:, 0:128], got[:, 128:256]
        q[rows, :] = high + low
        own_hl[rows, 0:128] = high.astype(BF16)
        own_hl[rows, 128:256] = low.astype(BF16)
        own_lh[rows, 0:128] = low.astype(BF16)
        own_lh[rows, 128:256] = high.astype(BF16)
        basis_h[rows, :] = got[:, 256:512].astype(BF16)
        basis_l[rows, :] = got[:, 512:768].astype(BF16)
        return carry

    lax.fori_loop(0, STEPS, reorder, 0)
    for i in range(STEPS):
        rows = pl.ds(i * BLOCK, BLOCK)
        near_q.append(send(q.at[rows], q_in.at[rows], (leaf, ahead)))

    leaf_coef = dot3((rhs_h[...], rhs_l[...]), (basis_h[...], basis_l[...]), FIRST)
    loads[3].wait()
    transfer_hl = split(transfer[0])
    lifted[...] = dot3(split(leaf_coef), transfer_hl).reshape(LEAVES // 2, 2, PART, RANK)
    halved = [send(lifted.at[:, 1 - core], half.at[:, 0], (leaf - step, wide))]

    def norms(points_ref, column, row):
        sq = SCALE * jnp.sum(points_ref[...] * points_ref[...], axis=1, keepdims=True)
        column[...] = sq
        row[...] = jnp.transpose(jnp.broadcast_to(sq, (sq.shape[0], 128)))[0:1, :]

    def tile(left, left_col, right_hl, right_lh, right_row, factor=None):
        cross = dot(left, right_hl, LAST) + dot(left, right_lh, LAST)
        t = jnp.exp2((left_col + right_row) - (2.0 * SCALE) * cross)
        return split(t if factor is None else factor * t)

    def own_term(i, carry):
        rows = pl.ds(pl.multiple_of(i * BLOCK, BLOCK), BLOCK)
        t = tile(own_hl[rows, :], own_col[rows, :], own_hl[...], own_lh[...], own_row[...])
        out[rows, :] = dot3(t, (rhs_h[...], rhs_l[...]))
        return carry

    norms(q, own_col, own_row)
    arrived(halved)
    half[:, 1] = half[:, 0] + lifted[:, core]
    pieces[chip] = half[chip, 1]
    piece = []
    for d in (2, 1, 3):
        other = lax.rem(chip + d, LEAVES // 2)
        piece.append(send(half.at[other, 1], pieces.at[chip], (2 * other + core, wide)))
    def set_of(d):
        return skels.at[lax.rem(chip + d, LEAVES // 2), core]

    arrived(skel_row)
    skel_up = send(own_set, own_set, leaf_peer(2))
    skel_down = send(own_set, own_set, leaf_peer(6))
    skel_inside = [send(own_set, own_set, partner)]
    lax.fori_loop(0, STEPS, own_term, 0)

    arrived(piece)
    coefs[z] = jnp.sum(pieces[...], axis=0)
    coef_row = {d: send(coefs.at[z], coefs.at[z], (leaf, z_index(d))) for d in FARTHEST_FIRST}
    send_rhs(2)

    arrived(near_q)
    high, low = split(q_in[...])
    in_hl[:, 0:128], in_hl[:, 128:256] = high, low
    in_lh[:, 0:128], in_lh[:, 128:256] = low, high
    norms(q_in, in_col, in_row)

    def share_term(i):
        rows = pl.ds(i * BLOCK, BLOCK)
        t = tile(in_hl[rows, :], in_col[rows, :], own_hl[...], own_lh[...], own_row[...])
        share_out[rows, :] = dot3(t, (rhs_h[...], rhs_l[...]))
        shares.append(send(share_out.at[rows], share_in.at[rows], (leaf, behind)))

    share_term(0)
    skel_down.wait_recv()
    skel_on = send(set_of(1), set_of(1), leaf_peer(6))
    skel_inside.append(send(set_of(1), set_of(1), partner))
    skel_up.wait_recv()
    skel_inside.append(send(set_of(3), set_of(3), partner))
    share_term(1)
    send_rhs(3)
    share_term(2)
    share_term(3)
    skel_on.wait_recv()
    skel_inside.append(send(set_of(2), set_of(2), partner))

    arrived(skel_inside)
    for i in range(NX):
        points_of = skels[:, :, NZ + i].reshape(RANK, FEAT)
        high, low = split(points_of)
        rows = pl.ds(i * RANK, RANK)
        far_hl[rows, 0:128], far_hl[rows, 128:256] = high, low
        far_lh[rows, 0:128], far_lh[rows, 128:256] = low, high
        far_points[rows, :] = points_of
    norms(far_points, far_col, far_row)

    def far_tile(i, carry):
        sources = skels[:, :, i].reshape(RANK, FEAT)
        source_sq = SCALE * jnp.sum(sources * sources, axis=1, keepdims=True)
        lists = []
        for k in range(NX):
            hits = jnp.float32(0.0)
            for j in range(FAR):
                target = k * NZ + z
                hit = (far_ids[j, target] == x * NZ + i) & (far_count[target] > j)
                hits += jnp.where(hit, 1.0, 0.0).astype(F32)
            lists.append(jnp.full((1, RANK), hits, F32))
        tile_h[i], tile_l[i] = tile(
            jnp.concatenate(split(sources), axis=1), source_sq, far_hl[...], far_lh[...], far_row[...],
            jnp.concatenate(lists, axis=1))
        return carry

    lax.fori_loop(0, NZ, far_tile, 0)

    def far_term(i):
        high, low = split(coefs[i])
        both = dot(jnp.concatenate([high, low], axis=0), tile_h[i])
        return both[:PART] + (both[PART:] + dot(high, tile_l[i]))

    total = far_term(z)
    for d in FARTHEST_FIRST[::-1]:
        coef_row[d].wait_recv()
        total += far_term(lax.rem(z - d + NZ, NZ))
    for i in range(NX):
        parts_out[i] = total[:, i * RANK:(i + 1) * RANK]
    parts = []
    for d in (2, 1, 3):
        parts.append(send(parts_out.at[lax.rem(x + d, NX)], parts_in.at[x], (leaf, x_index(d) + z)))
    parts_in[x] = parts_out[x]

    first_id, second_id, used = near_ids[0, 0], near_ids[0, 1], near_count[0]
    number = leaf * WIDE + wide

    def listed(other):
        return jnp.where(((first_id == other) & (used > 0)) | ((second_id == other) & (used > 1)), 1.0, 0.0).astype(F32)

    behind_used, ahead_used = listed(number - step), listed(number + step)

    arrived(near_rhs)
    in_h[...], in_l[...] = split(rhs_in[...])

    def near_term(i, carry):
        rows = pl.ds(pl.multiple_of(i * BLOCK, BLOCK), BLOCK)
        t = tile(own_hl[rows, :], own_col[rows, :], in_hl[...], in_lh[...], in_row[...])
        out[rows, :] += behind_used * dot3(t, (in_h[...], in_l[...]))
        return carry

    lax.fori_loop(0, STEPS, near_term, 0)

    arrived(parts)
    total = jnp.sum(parts_in[...], axis=0)
    field[chip, core] = total
    fields = [send(field.at[chip, core], field.at[chip, core], leaf_peer(d)) for d in (4, 2, 6)]
    inside = [send(field.at[chip, core], field.at[chip, core], partner)]
    arrived(shares)
    share[...] = ahead_used * share_in[...]
    for copy, d in ((fields[1], 2), (fields[2], 6), (fields[0], 4)):
        copy.wait_recv()
        block = field.at[lax.rem(chip + LEAVES // 2 - d // 2, LEAVES // 2), core]
        inside.append(send(block, block, partner))
    arrived(inside)
    leaf_field = dot3(split(field[...].reshape(COLS, RANK)), transfer_hl, LAST)
    out[...] += dot3((basis_h[...], basis_l[...]), split(leaf_field), LAST)
    for copy in copies:
        copy.wait_send()


def shards(rhs, points, order, basis, transfer, skeleton, far_ids, far_count, near_ids, near_count):
    vmem, smem, anywhere = (pl.BlockSpec(memory_space=m) for m in (pltpu.VMEM, pltpu.SMEM, pl.ANY))

    def held(*shape, dtype=F32):
        return pltpu.VMEM(shape, dtype)

    wide_bf16 = held(ROWS, 256, dtype=BF16)
    total, share = pl.pallas_call(
        kernel,
        out_shape=(jax.ShapeDtypeStruct((ROWS, COLS), F32), jax.ShapeDtypeStruct((ROWS, COLS), F32)),
        in_specs=[vmem, smem, smem, smem, smem] + [anywhere] * 4 + [vmem],
        out_specs=(vmem, vmem),
        scratch_shapes=[
            held(ROWS, COLS), held(ROWS, FEAT), held(ROWS, RANK), held(1, RANK, RANK),
            held(ROWS, 768, dtype=BF16),
            held(ROWS, FEAT), wide_bf16, wide_bf16, held(ROWS, 1), held(1, ROWS),
            held(ROWS, FEAT), wide_bf16, wide_bf16, held(ROWS, 1), held(1, ROWS),
            wide_bf16, wide_bf16, wide_bf16, wide_bf16,
            held(ROWS, COLS), wide_bf16, wide_bf16,
            held(ROWS, COLS), held(ROWS, COLS),
            held(LEAVES // 2, 2, PART, RANK), held(LEAVES // 2, 2, PART, RANK),
            held(LEAVES // 2, PART, RANK), held(NZ, PART, RANK),
            held(LEAVES // 2, 2, NZ + NX, PART, FEAT),
            held(NX * RANK, FEAT), wide_bf16, wide_bf16, held(ROWS, 1), held(1, ROWS),
            held(NZ, RANK, NX * RANK, dtype=BF16), held(NZ, RANK, NX * RANK, dtype=BF16),
            held(NX, PART, RANK), held(NX, PART, RANK),
            held(LEAVES // 2, 2, PART, RANK),
            pltpu.SemaphoreType.DMA((4,)),
            pltpu.SemaphoreType.DMA((COPIES,)),
            pltpu.SemaphoreType.DMA((COPIES,)),
        ],
        compiler_params=pltpu.CompilerParams(
            collective_id=0, has_side_effects=True, vmem_limit_bytes=56 * 1024 * 1024),
    )(order.reshape(1, ROWS), far_ids.T, far_count, near_ids, near_count, rhs, points, basis, transfer, skeleton)
    return total + share


def solution(mesh):
    placed = (
        P(("leaf", "wide"), None),
        P(("leaf", "wide"), None),
        P(("leaf", "wide")),
        P(("leaf", "wide"), None),
        P(("leaf", "wide"), None, None),
        P("wide", "leaf", None),
        P(),
        P(),
        P(("leaf", "wide"), None),
        P(("leaf", "wide")),
    )
    return jax.shard_map(
        shards, mesh=mesh, in_specs=placed, out_specs=P(("leaf", "wide"), None), check_vma=False
    )
```

```python
import jax
import jax.numpy as jnp
from jax import lax
from jax.experimental import pallas as pl
from jax.experimental.pallas import tpu as pltpu
from jax.sharding import PartitionSpec as P

MESH = pl.DeviceIdType.MESH
F32, BF16 = jnp.float32, jnp.bfloat16
LEAVES, WIDE, NX, NZ = 8, 32, 4, 8
ROWS, FEAT, RANK, COLS = 1024, 128, 256, 256
FAR, PART = 6, 32
BLOCK = 256
STEPS = ROWS // BLOCK
RHS_CHUNK = 128
COPIES = 128
SCALE = -(2.0 / FEAT) * 1.4426950408889634

LAST = (((1,), (1,)), ((), ()))
FIRST = (((0,), (0,)), ((), ()))
PLAIN = (((1,), (0,)), ((), ()))
FARTHEST_FIRST = (4, 3, -3, 2, -2, 1, -1)


def dot(a, b, dims=PLAIN):
    return lax.dot_general(a, b, dims, preferred_element_type=F32)


def split(x):
    high = x.astype(BF16)
    return high, (x - high.astype(F32)).astype(BF16)


def dot3(a, b, dims=PLAIN):
    return dot(a[0], b[0], dims) + (dot(a[0], b[1], dims) + dot(a[1], b[0], dims))


def kernel(
    order, far_ids, far_count, near_ids, near_count, rhs_hbm, points_hbm, basis_hbm, transfer_hbm, skeleton,
    out, share_in, field, transfer_out, basis_h, basis_l, used_out,
    rhs, points, basis, transfer,
    moved, q, own_hl, own_lh, own_col, own_row, q_in, in_hl, in_lh, in_col, in_row,
    rhs_h, rhs_l, rhs_in, in_h, in_l, share_out,
    lifted, half, pieces, coefs, skels, far_points, far_hl, far_lh, far_col, far_row, tile_h, tile_l,
    parts_out, parts_in,
    load_sems, send_sems, recv_sems,
):
    leaf, wide = lax.axis_index("leaf"), lax.axis_index("wide")
    core, chip = lax.rem(leaf, 2), lax.div(leaf, 2)
    x, z = lax.div(wide, NZ), lax.rem(wide, NZ)
    step = 2 * core - 1
    ahead, behind = lax.rem(wide + step + WIDE, WIDE), lax.rem(wide - step + WIDE, WIDE)

    def leaf_peer(d):
        return lax.rem(leaf + d, LEAVES), wide

    def z_index(d):
        return x * NZ + lax.rem(z + d + NZ, NZ)

    def x_index(d):
        return lax.rem(x + d + 3 * NX, NX) * NZ

    loads = []
    for source, target in ((rhs_hbm, rhs), (points_hbm, points), (basis_hbm, basis), (transfer_hbm, transfer)):
        load = pltpu.make_async_copy(source, target, load_sems.at[len(loads)])
        load.start()
        loads.append(load)

    barrier = pltpu.get_barrier_semaphore()
    partners = [leaf_peer(d) for d in range(1, LEAVES)] + [(leaf, z_index(d)) for d in range(1, NZ)]
    partners += [(leaf, x_index(d) + z) for d in range(1, NX)] + [(leaf, ahead), (leaf, behind)]
    for partner in partners:
        pl.semaphore_signal(barrier, inc=1, device_id=partner, device_id_type=MESH)
    pl.semaphore_wait(barrier, len(partners))

    copies = []

    def send(src, dst, partner):
        k = len(copies)
        copy = pltpu.make_async_remote_copy(
            src_ref=src, dst_ref=dst, send_sem=send_sems.at[k], recv_sem=recv_sems.at[k],
            device_id=partner, device_id_type=MESH)
        copy.start()
        copies.append(copy)
        return copy

    def arrived(group):
        for copy in group:
            copy.wait_recv()

    FARTHEST_FIRST = (4, 3, -3, 2, -2, 1, -1)

    own_set = skels.at[chip, core]
    partner = (leaf - step, wide)
    skel_row = [send(skeleton.at[0], own_set.at[z], (leaf, z_index(d))) for d in FARTHEST_FIRST]
    skel_row += [send(skeleton.at[0], own_set.at[NZ + x], (leaf, x_index(d) + z)) for d in (2, 1, 3)]
    skels[chip, core, z] = skeleton[0]
    skels[chip, core, NZ + x] = skeleton[0]

    near_rhs, near_q, shares = [], [], []

    def send_rhs(count):
        for _ in range(count):
            rows = pl.ds(len(near_rhs) * RHS_CHUNK, RHS_CHUNK)
            near_rhs.append(send(rhs.at[rows], rhs_in.at[rows], (leaf, ahead)))

    loads[0].wait()
    send_rhs(3)
    rhs_h[...], rhs_l[...] = split(rhs[...])
    loads[1].wait()
    loads[2].wait()

    moved[:, 0:128], moved[:, 128:256] = split(points[...])
    moved[:, 256:512], moved[:, 512:768] = split(basis[...])

    def reorder(i, carry):
        rows = pl.ds(pl.multiple_of(i * BLOCK, BLOCK), BLOCK)
        place = lax.broadcasted_iota(jnp.int32, (BLOCK, ROWS), 0) + i * BLOCK
        chosen_rows = jnp.where(order[...] == place, 1.0, 0.0).astype(BF16)
        got = dot(chosen_rows, moved[...])
        high, low = got[:, 0:128], got[:, 128:256]
        q[rows, :] = high + low
        own_hl[rows, 0:128] = high.astype(BF16)
        own_hl[rows, 128:256] = low.astype(BF16)
        own_lh[rows, 0:128] = low.astype(BF16)
        own_lh[rows, 128:256] = high.astype(BF16)
        basis_h[rows, :] = got[:, 256:512].astype(BF16)
        basis_l[rows, :] = got[:, 512:768].astype(BF16)
        return carry

    lax.fori_loop(0, STEPS, reorder, 0)
    for i in range(STEPS):
        rows = pl.ds(i * BLOCK, BLOCK)
        near_q.append(send(q.at[rows], q_in.at[rows], (leaf, ahead)))

    leaf_coef = dot3((rhs_h[...], rhs_l[...]), (basis_h[...], basis_l[...]), FIRST)
    loads[3].wait()
    transfer_out[...] = transfer[0]
    transfer_hl = split(transfer[0])
    lifted[...] = dot3(split(leaf_coef), transfer_hl).reshape(LEAVES // 2, 2, PART, RANK)
    halved = [send(lifted.at[:, 1 - core], half.at[:, 0], (leaf - step, wide))]

    def norms(points_ref, column, row):
        sq = SCALE * jnp.sum(points_ref[...] * points_ref[...], axis=1, keepdims=True)
        column[...] = sq
        row[...] = jnp.transpose(jnp.broadcast_to(sq, (sq.shape[0], 128)))[0:1, :]

    def tile(left, left_col, right_hl, right_lh, right_row, factor=None):
        cross = dot(left, right_hl, LAST) + dot(left, right_lh, LAST)
        t = jnp.exp2((left_col + right_row) - (2.0 * SCALE) * cross)
        return split(t if factor is None else factor * t)

    def own_term(i, carry):
        rows = pl.ds(pl.multiple_of(i * BLOCK, BLOCK), BLOCK)
        t = tile(own_hl[rows, :], own_col[rows, :], own_hl[...], own_lh[...], own_row[...])
        out[rows, :] = dot3(t, (rhs_h[...], rhs_l[...]))
        return carry

    norms(q, own_col, own_row)
    arrived(halved)
    half[:, 1] = half[:, 0] + lifted[:, core]
    pieces[chip] = half[chip, 1]
    piece = []
    for d in (2, 1, 3):
        other = lax.rem(chip + d, LEAVES // 2)
        piece.append(send(half.at[other, 1], pieces.at[chip], (2 * other + core, wide)))
    def set_of(d):
        return skels.at[lax.rem(chip + d, LEAVES // 2), core]

    arrived(skel_row)
    skel_up = send(own_set, own_set, leaf_peer(2))
    skel_down = send(own_set, own_set, leaf_peer(6))
    skel_inside = [send(own_set, own_set, partner)]
    lax.fori_loop(0, STEPS, own_term, 0)

    arrived(piece)
    coefs[z] = jnp.sum(pieces[...], axis=0)
    coef_row = {d: send(coefs.at[z], coefs.at[z], (leaf, z_index(d))) for d in FARTHEST_FIRST}
    send_rhs(2)

    arrived(near_q)
    high, low = split(q_in[...])
    in_hl[:, 0:128], in_hl[:, 128:256] = high, low
    in_lh[:, 0:128], in_lh[:, 128:256] = low, high
    norms(q_in, in_col, in_row)

    def share_term(i):
        rows = pl.ds(i * BLOCK, BLOCK)
        t = tile(in_hl[rows, :], in_col[rows, :], own_hl[...], own_lh[...], own_row[...])
        share_out[rows, :] = dot3(t, (rhs_h[...], rhs_l[...]))
        shares.append(send(share_out.at[rows], share_in.at[rows], (leaf, behind)))

    share_term(0)
    skel_down.wait_recv()
    skel_on = send(set_of(1), set_of(1), leaf_peer(6))
    skel_inside.append(send(set_of(1), set_of(1), partner))
    skel_up.wait_recv()
    skel_inside.append(send(set_of(3), set_of(3), partner))
    share_term(1)
    send_rhs(3)
    share_term(2)
    share_term(3)
    skel_on.wait_recv()
    skel_inside.append(send(set_of(2), set_of(2), partner))

    arrived(skel_inside)
    for i in range(NX):
        points_of = skels[:, :, NZ + i].reshape(RANK, FEAT)
        high, low = split(points_of)
        rows = pl.ds(i * RANK, RANK)
        far_hl[rows, 0:128], far_hl[rows, 128:256] = high, low
        far_lh[rows, 0:128], far_lh[rows, 128:256] = low, high
        far_points[rows, :] = points_of
    norms(far_points, far_col, far_row)

    def far_tile(i, carry):
        sources = skels[:, :, i].reshape(RANK, FEAT)
        source_sq = SCALE * jnp.sum(sources * sources, axis=1, keepdims=True)
        lists = []
        for k in range(NX):
            hits = jnp.float32(0.0)
            for j in range(FAR):
                target = k * NZ + z
                hit = (far_ids[j, target] == x * NZ + i) & (far_count[target] > j)
                hits += jnp.where(hit, 1.0, 0.0).astype(F32)
            lists.append(jnp.full((1, RANK), hits, F32))
        tile_h[i], tile_l[i] = tile(
            jnp.concatenate(split(sources), axis=1), source_sq, far_hl[...], far_lh[...], far_row[...],
            jnp.concatenate(lists, axis=1))
        return carry

    lax.fori_loop(0, NZ, far_tile, 0)

    def far_term(i):
        high, low = split(coefs[i])
        both = dot(jnp.concatenate([high, low], axis=0), tile_h[i])
        return both[:PART] + (both[PART:] + dot(high, tile_l[i]))

    total = far_term(z)
    for d in FARTHEST_FIRST[::-1]:
        coef_row[d].wait_recv()
        total += far_term(lax.rem(z - d + NZ, NZ))
    for i in range(NX):
        parts_out[i] = total[:, i * RANK:(i + 1) * RANK]
    parts = []
    for d in (2, 1, 3):
        parts.append(send(parts_out.at[lax.rem(x + d, NX)], parts_in.at[x], (leaf, x_index(d) + z)))
    parts_in[x] = parts_out[x]

    first_id, second_id, used = near_ids[0, 0], near_ids[0, 1], near_count[0]
    number = leaf * WIDE + wide

    def listed(other):
        return jnp.where(((first_id == other) & (used > 0)) | ((second_id == other) & (used > 1)), 1.0, 0.0).astype(F32)

    behind_used, ahead_used = listed(number - step), listed(number + step)

    used_out[...] = jnp.full(used_out.shape, ahead_used, F32)
    arrived(near_rhs)
    in_h[...], in_l[...] = split(rhs_in[...])

    def near_term(i, carry):
        rows = pl.ds(pl.multiple_of(i * BLOCK, BLOCK), BLOCK)
        t = tile(own_hl[rows, :], own_col[rows, :], in_hl[...], in_lh[...], in_row[...])
        out[rows, :] += behind_used * dot3(t, (in_h[...], in_l[...]))
        return carry

    lax.fori_loop(0, STEPS, near_term, 0)

    arrived(parts)
    total = jnp.sum(parts_in[...], axis=0)
    field[chip, core] = total
    fields = [send(field.at[chip, core], field.at[chip, core], leaf_peer(d)) for d in (4, 2, 6)]
    inside = [send(field.at[chip, core], field.at[chip, core], partner)]
    arrived(shares)
    for copy, d in ((fields[1], 2), (fields[2], 6), (fields[0], 4)):
        copy.wait_recv()
        block = field.at[lax.rem(chip + LEAVES // 2 - d // 2, LEAVES // 2), core]
        inside.append(send(block, block, partner))
    arrived(inside)
    for copy in copies:
        copy.wait_send()


def finish(total, share, field, transfer, basis_h, basis_l, used, out, block, sems):
    leaf_field = dot3(split(field[...].reshape(COLS, RANK)), split(transfer[...]), LAST)
    leaf_field_hl = split(leaf_field)
    copies = []
    for i in range(STEPS):
        rows = pl.ds(i * BLOCK, BLOCK)
        far = dot3((basis_h[rows, :], basis_l[rows, :]), leaf_field_hl, LAST)
        block[rows, :] = total[rows, :] + (far + used[0:1, 0:1] * share[rows, :])
        copies.append(pltpu.make_async_copy(block.at[rows], out.at[rows], sems.at[i]))
        copies[-1].start()
    for copy in copies:
        copy.wait()


def shards(rhs, points, order, basis, transfer, skeleton, far_ids, far_count, near_ids, near_count):
    vmem, smem, anywhere = (pl.BlockSpec(memory_space=m) for m in (pltpu.VMEM, pltpu.SMEM, pl.ANY))

    def held(*shape, dtype=F32):
        return pltpu.VMEM(shape, dtype)

    wide_bf16 = held(ROWS, 256, dtype=BF16)
    left = [
        pltpu.VMEM((ROWS, COLS), F32), pltpu.VMEM((ROWS, COLS), F32), pltpu.VMEM((LEAVES // 2, 2, PART, RANK), F32),
        pltpu.VMEM((RANK, RANK), F32), wide_bf16, wide_bf16, pltpu.VMEM((8, 128), F32)]
    pieces = pl.pallas_call(
        kernel,
        out_shape=left,
        in_specs=[vmem, smem, smem, smem, smem] + [anywhere] * 4 + [vmem],
        out_specs=[vmem] * len(left),
        scratch_shapes=[
            held(ROWS, COLS), held(ROWS, FEAT), held(ROWS, RANK), held(1, RANK, RANK),
            held(ROWS, 768, dtype=BF16),
            held(ROWS, FEAT), wide_bf16, wide_bf16, held(ROWS, 1), held(1, ROWS),
            held(ROWS, FEAT), wide_bf16, wide_bf16, held(ROWS, 1), held(1, ROWS),
            wide_bf16, wide_bf16,
            held(ROWS, COLS), wide_bf16, wide_bf16,
            held(ROWS, COLS),
            held(LEAVES // 2, 2, PART, RANK), held(LEAVES // 2, 2, PART, RANK),
            held(LEAVES // 2, PART, RANK), held(NZ, PART, RANK),
            held(LEAVES // 2, 2, NZ + NX, PART, FEAT),
            held(NX * RANK, FEAT), wide_bf16, wide_bf16, held(ROWS, 1), held(1, ROWS),
            held(NZ, RANK, NX * RANK, dtype=BF16), held(NZ, RANK, NX * RANK, dtype=BF16),
            held(NX, PART, RANK), held(NX, PART, RANK),
            pltpu.SemaphoreType.DMA((4,)),
            pltpu.SemaphoreType.DMA((COPIES,)),
            pltpu.SemaphoreType.DMA((COPIES,)),
        ],
        compiler_params=pltpu.CompilerParams(
            collective_id=0, has_side_effects=True, vmem_limit_bytes=63000000),
    )(order.reshape(1, ROWS), far_ids.T, far_count, near_ids, near_count, rhs, points, basis, transfer, skeleton)
    return pl.pallas_call(
        finish,
        out_shape=jax.ShapeDtypeStruct((ROWS, COLS), F32),
        in_specs=[vmem] * len(left),
        out_specs=anywhere,
        scratch_shapes=[held(ROWS, COLS), pltpu.SemaphoreType.DMA((STEPS,))],
        compiler_params=pltpu.CompilerParams(vmem_limit_bytes=16 * 1024 * 1024),
    )(*[pltpu.with_memory_space_constraint(piece, pltpu.VMEM) for piece in pieces])


def solution(mesh):
    placed = (
        P(("leaf", "wide"), None),
        P(("leaf", "wide"), None),
        P(("leaf", "wide")),
        P(("leaf", "wide"), None),
        P(("leaf", "wide"), None, None),
        P("wide", "leaf", None),
        P(),
        P(),
        P(("leaf", "wide"), None),
        P(("leaf", "wide")),
    )
    return jax.shard_map(
        shards, mesh=mesh, in_specs=placed, out_specs=P(("leaf", "wide"), None), check_vma=False
    )
```

```python
import jax
import jax.numpy as jnp
from jax import lax
from jax.experimental import pallas as pl
from jax.experimental.pallas import tpu as pltpu
from jax.sharding import PartitionSpec as P

MESH = pl.DeviceIdType.MESH
F32, BF16 = jnp.float32, jnp.bfloat16
LEAVES, WIDE, NX, NZ = 8, 32, 4, 8
ROWS, FEAT, RANK, COLS = 1024, 128, 256, 256
FAR, PART = 6, 32
BLOCK = 256
STEPS = ROWS // BLOCK
RHS_CHUNK = 128
COPIES = 128
SCALE = -(2.0 / FEAT) * 1.4426950408889634

LAST = (((1,), (1,)), ((), ()))
FIRST = (((0,), (0,)), ((), ()))
PLAIN = (((1,), (0,)), ((), ()))
FARTHEST_FIRST = (-2, 3, -3, 2, 1, -1)


def dot(a, b, dims=PLAIN):
    return lax.dot_general(a, b, dims, preferred_element_type=F32)


def split(x):
    high = x.astype(BF16)
    return high, (x - high.astype(F32)).astype(BF16)


def dot3(a, b, dims=PLAIN):
    return dot(a[0], b[0], dims) + (dot(a[0], b[1], dims) + dot(a[1], b[0], dims))


def kernel(
    order, far_ids, far_count, near_ids, near_count, rhs_hbm, points_hbm, basis_hbm, transfer_hbm, skeleton,
    out, share_in, field, transfer_out, basis_h, basis_l, used_out,
    rhs, points, basis, transfer,
    moved, q, own_hl, own_lh, own_col, own_row, q_in, in_hl, in_lh, in_col, in_row,
    rhs_h, rhs_l, rhs_in, in_h, in_l, share_out,
    lifted, half, pieces, coefs, skels, far_points, far_hl, far_lh, far_col, far_row, tile_h, tile_l,
    parts_out, parts_in,
    load_sems, send_sems, recv_sems,
):
    leaf, wide = lax.axis_index("leaf"), lax.axis_index("wide")
    core, chip = lax.rem(leaf, 2), lax.div(leaf, 2)
    x, z = lax.div(wide, NZ), lax.rem(wide, NZ)
    step = 2 * core - 1
    ahead, behind = lax.rem(wide + step + WIDE, WIDE), lax.rem(wide - step + WIDE, WIDE)

    def leaf_peer(d):
        return lax.rem(leaf + d, LEAVES), wide

    def z_index(d):
        return x * NZ + lax.rem(z + d + NZ, NZ)

    def x_index(d):
        return lax.rem(x + d + 3 * NX, NX) * NZ

    loads = []
    for source, target in ((rhs_hbm, rhs), (points_hbm, points), (basis_hbm, basis), (transfer_hbm, transfer)):
        load = pltpu.make_async_copy(source, target, load_sems.at[len(loads)])
        load.start()
        loads.append(load)

    barrier = pltpu.get_barrier_semaphore()
    partners = [leaf_peer(d) for d in range(1, LEAVES)] + [(leaf, z_index(d)) for d in range(1, NZ)]
    partners += [(leaf, x_index(d) + z) for d in range(1, NX)] + [(leaf, ahead), (leaf, behind)]
    for partner in partners:
        pl.semaphore_signal(barrier, inc=1, device_id=partner, device_id_type=MESH)
    pl.semaphore_wait(barrier, len(partners))

    copies = []

    def send(src, dst, partner):
        k = len(copies)
        copy = pltpu.make_async_remote_copy(
            src_ref=src, dst_ref=dst, send_sem=send_sems.at[k], recv_sem=recv_sems.at[k],
            device_id=partner, device_id_type=MESH)
        copy.start()
        copies.append(copy)
        return copy

    def arrived(group):
        for copy in group:
            copy.wait_recv()


    own_set = skels.at[chip, core]
    partner = (leaf - step, wide)
    skel_row = [send(skeleton.at[0], own_set.at[z], (leaf, z_index(d))) for d in (4,) + FARTHEST_FIRST]
    skel_row += [send(skeleton.at[0], own_set.at[NZ + x], (leaf, x_index(d) + z)) for d in (2, 1, 3)]
    skels[chip, core, z] = skeleton[0]
    skels[chip, core, NZ + x] = skeleton[0]

    near_rhs, near_q, shares = [], [], []

    def send_rhs(count):
        for _ in range(count):
            rows = pl.ds(len(near_rhs) * RHS_CHUNK, RHS_CHUNK)
            near_rhs.append(send(rhs.at[rows], rhs_in.at[rows], (leaf, ahead)))

    loads[0].wait()
    send_rhs(3)
    rhs_h[...], rhs_l[...] = split(rhs[...])
    loads[1].wait()
    loads[2].wait()

    moved[:, 0:128], moved[:, 128:256] = split(points[...])
    moved[:, 256:512], moved[:, 512:768] = split(basis[...])

    def reorder(i, carry):
        rows = pl.ds(pl.multiple_of(i * BLOCK, BLOCK), BLOCK)
        place = lax.broadcasted_iota(jnp.int32, (BLOCK, ROWS), 0) + i * BLOCK
        chosen_rows = jnp.where(order[...] == place, 1.0, 0.0).astype(BF16)
        got = dot(chosen_rows, moved[...])
        high, low = got[:, 0:128], got[:, 128:256]
        q[rows, :] = high + low
        own_hl[rows, 0:128] = high.astype(BF16)
        own_hl[rows, 128:256] = low.astype(BF16)
        own_lh[rows, 0:128] = low.astype(BF16)
        own_lh[rows, 128:256] = high.astype(BF16)
        basis_h[rows, :] = got[:, 256:512].astype(BF16)
        basis_l[rows, :] = got[:, 512:768].astype(BF16)
        return carry

    lax.fori_loop(0, STEPS, reorder, 0)
    for i in range(STEPS):
        rows = pl.ds(i * BLOCK, BLOCK)
        near_q.append(send(q.at[rows], q_in.at[rows], (leaf, ahead)))

    leaf_coef = dot3((rhs_h[...], rhs_l[...]), (basis_h[...], basis_l[...]), FIRST)
    loads[3].wait()
    transfer_out[...] = transfer[0]
    transfer_hl = split(transfer[0])
    lifted[...] = dot3(split(leaf_coef), transfer_hl).reshape(LEAVES // 2, 2, PART, RANK)
    halved = [send(lifted.at[:, 1 - core], half.at[:, 0], (leaf - step, wide))]

    def norms(points_ref, column, row):
        sq = SCALE * jnp.sum(points_ref[...] * points_ref[...], axis=1, keepdims=True)
        column[...] = sq
        row[...] = jnp.transpose(jnp.broadcast_to(sq, (sq.shape[0], 128)))[0:1, :]

    def tile(left, left_col, right_hl, right_lh, right_row, factor=None):
        cross = dot(left, right_hl, LAST) + dot(left, right_lh, LAST)
        t = jnp.exp2((left_col + right_row) - (2.0 * SCALE) * cross)
        return split(t if factor is None else factor * t)

    def own_term(i, carry):
        rows = pl.ds(pl.multiple_of(i * BLOCK, BLOCK), BLOCK)
        t = tile(own_hl[rows, :], own_col[rows, :], own_hl[...], own_lh[...], own_row[...])
        out[rows, :] = dot3(t, (rhs_h[...], rhs_l[...]))
        return carry

    norms(q, own_col, own_row)
    arrived(halved)
    half[:, 1] = half[:, 0] + lifted[:, core]
    pieces[chip] = half[chip, 1]
    piece = []
    for d in (2, 1, 3):
        other = lax.rem(chip + d, LEAVES // 2)
        piece.append(send(half.at[other, 1], pieces.at[chip], (2 * other + core, wide)))
    def set_of(d):
        return skels.at[lax.rem(chip + d, LEAVES // 2), core]

    arrived(skel_row)
    skel_up = send(own_set, own_set, leaf_peer(2))
    skel_down = send(own_set, own_set, leaf_peer(6))
    skel_inside = [send(own_set, own_set, partner)]
    lax.fori_loop(0, STEPS, own_term, 0)

    arrived(piece)
    coefs[z] = jnp.sum(pieces[...], axis=0)
    coef_row = {d: send(coefs.at[z], coefs.at[z], (leaf, z_index(d))) for d in FARTHEST_FIRST}
    send_rhs(2)

    arrived(near_q)
    high, low = split(q_in[...])
    in_hl[:, 0:128], in_hl[:, 128:256] = high, low
    in_lh[:, 0:128], in_lh[:, 128:256] = low, high
    norms(q_in, in_col, in_row)

    def share_term(i):
        rows = pl.ds(i * BLOCK, BLOCK)
        t = tile(in_hl[rows, :], in_col[rows, :], own_hl[...], own_lh[...], own_row[...])
        share_out[rows, :] = dot3(t, (rhs_h[...], rhs_l[...]))
        shares.append(send(share_out.at[rows], share_in.at[rows], (leaf, behind)))

    share_term(0)
    coef_row[-2].wait_recv()
    block = coefs.at[lax.rem(z + 2, NZ)]
    coef_row[4] = send(block, block, (leaf, z_index(-2)))
    skel_down.wait_recv()
    skel_on = send(set_of(1), set_of(1), leaf_peer(6))
    skel_inside.append(send(set_of(1), set_of(1), partner))
    skel_up.wait_recv()
    skel_inside.append(send(set_of(3), set_of(3), partner))
    share_term(1)
    send_rhs(3)
    share_term(2)
    share_term(3)
    skel_on.wait_recv()
    skel_inside.append(send(set_of(2), set_of(2), partner))

    arrived(skel_inside)
    for i in range(NX):
        points_of = skels[:, :, NZ + i].reshape(RANK, FEAT)
        high, low = split(points_of)
        rows = pl.ds(i * RANK, RANK)
        far_hl[rows, 0:128], far_hl[rows, 128:256] = high, low
        far_lh[rows, 0:128], far_lh[rows, 128:256] = low, high
        far_points[rows, :] = points_of
    norms(far_points, far_col, far_row)

    def far_tile(i, carry):
        sources = skels[:, :, i].reshape(RANK, FEAT)
        source_sq = SCALE * jnp.sum(sources * sources, axis=1, keepdims=True)
        lists = []
        for k in range(NX):
            hits = jnp.float32(0.0)
            for j in range(FAR):
                target = k * NZ + z
                hit = (far_ids[j, target] == x * NZ + i) & (far_count[target] > j)
                hits += jnp.where(hit, 1.0, 0.0).astype(F32)
            lists.append(jnp.full((1, RANK), hits, F32))
        tile_h[i], tile_l[i] = tile(
            jnp.concatenate(split(sources), axis=1), source_sq, far_hl[...], far_lh[...], far_row[...],
            jnp.concatenate(lists, axis=1))
        return carry

    lax.fori_loop(0, NZ, far_tile, 0)

    def far_term(i):
        high, low = split(coefs[i])
        both = dot(jnp.concatenate([high, low], axis=0), tile_h[i])
        return both[:PART] + (both[PART:] + dot(high, tile_l[i]))

    total = far_term(z)
    for d in (-2, 1, -1, 2, 3, -3, 4):
        if d != -2:
            coef_row[d].wait_recv()
        total += far_term(lax.rem(z - d + NZ, NZ))
    for i in range(NX):
        parts_out[i] = total[:, i * RANK:(i + 1) * RANK]
    parts = []
    for d in (2, 1, 3):
        parts.append(send(parts_out.at[lax.rem(x + d, NX)], parts_in.at[x], (leaf, x_index(d) + z)))
    parts_in[x] = parts_out[x]

    first_id, second_id, used = near_ids[0, 0], near_ids[0, 1], near_count[0]
    number = leaf * WIDE + wide

    def listed(other):
        return jnp.where(((first_id == other) & (used > 0)) | ((second_id == other) & (used > 1)), 1.0, 0.0).astype(F32)

    behind_used, ahead_used = listed(number - step), listed(number + step)

    used_out[...] = jnp.full(used_out.shape, ahead_used, F32)
    arrived(near_rhs)
    in_h[...], in_l[...] = split(rhs_in[...])

    def near_term(i, carry):
        rows = pl.ds(pl.multiple_of(i * BLOCK, BLOCK), BLOCK)
        t = tile(own_hl[rows, :], own_col[rows, :], in_hl[...], in_lh[...], in_row[...])
        out[rows, :] += behind_used * dot3(t, (in_h[...], in_l[...]))
        return carry

    lax.fori_loop(0, STEPS, near_term, 0)

    arrived(parts)
    total = jnp.sum(parts_in[...], axis=0)
    field[chip, core] = total
    fields = [send(field.at[chip, core], field.at[chip, core], leaf_peer(d)) for d in (4, 2, 6)]
    inside = [send(field.at[chip, core], field.at[chip, core], partner)]
    arrived(shares)
    for copy, d in ((fields[1], 2), (fields[2], 6), (fields[0], 4)):
        copy.wait_recv()
        block = field.at[lax.rem(chip + LEAVES // 2 - d // 2, LEAVES // 2), core]
        inside.append(send(block, block, partner))
    arrived(inside)
    for copy in copies:
        copy.wait_send()


def finish(total, share, field, transfer, basis_h, basis_l, used, out, block, sems):
    leaf_field = dot3(split(field[...].reshape(COLS, RANK)), split(transfer[...]), LAST)
    leaf_field_hl = split(leaf_field)
    copies = []
    for i in range(STEPS):
        rows = pl.ds(i * BLOCK, BLOCK)
        far = dot3((basis_h[rows, :], basis_l[rows, :]), leaf_field_hl, LAST)
        block[rows, :] = total[rows, :] + (far + used[0:1, 0:1] * share[rows, :])
        copies.append(pltpu.make_async_copy(block.at[rows], out.at[rows], sems.at[i]))
        copies[-1].start()
    for copy in copies:
        copy.wait()


def shards(rhs, points, order, basis, transfer, skeleton, far_ids, far_count, near_ids, near_count):
    vmem, smem, anywhere = (pl.BlockSpec(memory_space=m) for m in (pltpu.VMEM, pltpu.SMEM, pl.ANY))

    def held(*shape, dtype=F32):
        return pltpu.VMEM(shape, dtype)

    wide_bf16 = held(ROWS, 256, dtype=BF16)
    left = [
        pltpu.VMEM((ROWS, COLS), F32), pltpu.VMEM((ROWS, COLS), F32), pltpu.VMEM((LEAVES // 2, 2, PART, RANK), F32),
        pltpu.VMEM((RANK, RANK), F32), wide_bf16, wide_bf16, pltpu.VMEM((8, 128), F32)]
    pieces = pl.pallas_call(
        kernel,
        out_shape=left,
        in_specs=[vmem, smem, smem, smem, smem] + [anywhere] * 4 + [vmem],
        out_specs=[vmem] * len(left),
        scratch_shapes=[
            held(ROWS, COLS), held(ROWS, FEAT), held(ROWS, RANK), held(1, RANK, RANK),
            held(ROWS, 768, dtype=BF16),
            held(ROWS, FEAT), wide_bf16, wide_bf16, held(ROWS, 1), held(1, ROWS),
            held(ROWS, FEAT), wide_bf16, wide_bf16, held(ROWS, 1), held(1, ROWS),
            wide_bf16, wide_bf16,
            held(ROWS, COLS), wide_bf16, wide_bf16,
            held(ROWS, COLS),
            held(LEAVES // 2, 2, PART, RANK), held(LEAVES // 2, 2, PART, RANK),
            held(LEAVES // 2, PART, RANK), held(NZ, PART, RANK),
            held(LEAVES // 2, 2, NZ + NX, PART, FEAT),
            held(NX * RANK, FEAT), wide_bf16, wide_bf16, held(ROWS, 1), held(1, ROWS),
            held(NZ, RANK, NX * RANK, dtype=BF16), held(NZ, RANK, NX * RANK, dtype=BF16),
            held(NX, PART, RANK), held(NX, PART, RANK),
            pltpu.SemaphoreType.DMA((4,)),
            pltpu.SemaphoreType.DMA((COPIES,)),
            pltpu.SemaphoreType.DMA((COPIES,)),
        ],
        compiler_params=pltpu.CompilerParams(
            collective_id=0, has_side_effects=True, vmem_limit_bytes=63000000),
    )(order.reshape(1, ROWS), far_ids.T, far_count, near_ids, near_count, rhs, points, basis, transfer, skeleton)
    return pl.pallas_call(
        finish,
        out_shape=jax.ShapeDtypeStruct((ROWS, COLS), F32),
        in_specs=[vmem] * len(left),
        out_specs=anywhere,
        scratch_shapes=[held(ROWS, COLS), pltpu.SemaphoreType.DMA((STEPS,))],
        compiler_params=pltpu.CompilerParams(vmem_limit_bytes=16 * 1024 * 1024),
    )(*[pltpu.with_memory_space_constraint(piece, pltpu.VMEM) for piece in pieces])


def solution(mesh):
    placed = (
        P(("leaf", "wide"), None),
        P(("leaf", "wide"), None),
        P(("leaf", "wide")),
        P(("leaf", "wide"), None),
        P(("leaf", "wide"), None, None),
        P("wide", "leaf", None),
        P(),
        P(),
        P(("leaf", "wide"), None),
        P(("leaf", "wide")),
    )
    return jax.shard_map(
        shards, mesh=mesh, in_specs=placed, out_specs=P(("leaf", "wide"), None), check_vma=False
    )
```
